8 devices in a mesh: dp: 1 (over z), a: 2 (over y), b: 4 (over x, core).
Axes of the slice: x: 2, y: 2, z: 1, core: 2. Of those that a mesh axis runs over, the one named last changes fastest.
Arguments:
- x: bfloat16 [2048, 8192], P('dp', ('a', 'b'))
- w_gate: bfloat16 [8192, 22016], P('a', 'b')
- w_up: bfloat16 [8192, 22016], P('a', 'b')
- w_down: bfloat16 [22016, 8192], P('b', 'a')
Outputs:
- output: bfloat16 [2048, 8192], P('dp', ('a', 'b'))
All inputs are finite; a program needn't handle non-finite values.
Results may differ from the reference program's by a relative error of at most 0.016.
Values are sent between devices in bfloat16 or wider.
A program may use at most 2 GiB of HBM per device.

```python
import jax
import jax.numpy as jnp

ROWS = 2048
D = 8192
FF = 22016


def setup_inputs(seed: int = 0, part: int = 0) -> dict:
    kx, kg, ku, kd = jax.random.split(jax.random.key(seed), 4)
    drawn = {
        "x": jax.random.normal(jax.random.fold_in(kx, part), (ROWS, D), jnp.float32),
        "w_gate": jax.random.normal(kg, (D, FF), jnp.float32) * D**-0.5,
        "w_up": jax.random.normal(ku, (D, FF), jnp.float32) * D**-0.5,
        "w_down": jax.random.normal(kd, (FF, D), jnp.float32) * FF**-0.5,
    }
    return {k: v.astype(jnp.bfloat16) for k, v in drawn.items()}


def reference(x, w_gate, w_up, w_down):
    gate = jnp.dot(x, w_gate, preferred_element_type=jnp.float32)
    up = jnp.dot(x, w_up, preferred_element_type=jnp.float32)
    hidden = (jax.nn.silu(gate) * up).astype(jnp.bfloat16)
    return jnp.dot(hidden, w_down, preferred_element_type=jnp.float32).astype(jnp.bfloat16)
```

```python
import jax
import jax.numpy as jnp
from jax import lax
from jax.sharding import PartitionSpec as P

SIZES = (128, 256, 256, 256, 128)


def solution(mesh):
    def body(x, w_gate, w_up, w_down):
        a = lax.axis_index("a")
        half = x.shape[0] // 2
        mine, other = a * half, (1 - a) * half
        swap = [(0, 1), (1, 0)]

        def gather(start, rows):
            part = lax.dynamic_slice_in_dim(x, start, rows, 0)
            return lax.all_gather(part, "b", axis=1, tiled=True)

        def dot(p, q):
            return jnp.dot(p, q, preferred_element_type=jnp.float32)

        def send(v):
            return lax.ppermute(v, "a", swap)

        y = jnp.zeros(x.shape, jnp.bfloat16)
        starts = [sum(SIZES[:i]) for i in range(len(SIZES))]

        def down(y, h, start):
            part = dot(h, w_down).astype(jnp.bfloat16)
            part = lax.psum_scatter(part, "b", scatter_dimension=1, tiled=True)
            return lax.dynamic_update_slice(y, part, (start, 0))

        arrived = []
        for o, n in zip(starts, SIZES):
            xr = gather(other + o, n)
            g = send(dot(xr, w_gate).astype(jnp.bfloat16))
            u = send(dot(xr, w_up).astype(jnp.bfloat16))
            arrived.append((g, u))
        hidden = []
        for (o, n), (g, u) in zip(zip(starts, SIZES), arrived):
            xl = gather(mine + o, n)
            g = dot(xl, w_gate) + g.astype(jnp.float32)
            u = dot(xl, w_up) + u.astype(jnp.float32)
            h = (jax.nn.silu(g) * u).astype(jnp.bfloat16)
            hidden.append((h, send(h)))
        for (o, n), (h, r) in zip(zip(starts, SIZES), hidden):
            y = down(y, h, mine + o)
            y = down(y, r, other + o)
        return y

    return jax.shard_map(
        body,
        mesh=mesh,
        in_specs=(P("dp", ("a", "b")), P("a", "b"), P("a", "b"), P("b", "a")),
        out_specs=P("dp", ("a", "b")),
        check_vma=False,
    )
```

```python
import functools

import jax
import jax.numpy as jnp
from jax import lax
from jax.experimental import pallas as pl
from jax.experimental.pallas import tpu as pltpu
from jax.sharding import PartitionSpec as P

BLOCK = 128
WIDE = 256
LANES = 128
LAG_E, LAG_D = 3, 6
RING = 8
KEPT = LAG_E + 1
WEIGHTS = 3
F32, BF16 = jnp.float32, jnp.bfloat16


def dot(p, q):
    return jnp.dot(p, q, preferred_element_type=F32)


def kernel(n, wide, x, wg, wu, wd, out, xg, wbuf, dbuf, acc, mine, psend, precv, hbuf, ysend, yrecv, yown, yout,
           x_own, x_send, x_recv, w_sem, d_sem, p_send, p_recv, q_send, q_recv, y_send, y_recv, o_sem):
    rows, depth = x.shape
    ff = wg.shape[1]
    half = rows // 2
    blocks = half // n
    tiles = -(-ff // wide)
    last = ff - (tiles - 1) * wide
    steps = blocks * tiles
    cut = depth
    a, b = lax.axis_index("a"), lax.axis_index("b")
    peers = [lax.rem(b + k, 4) for k in range(4)]
    partner = {"a": 1 - a}

    def rows_of(s, part):
        owner = a if part == 0 else 1 - a
        return pl.ds(pl.multiple_of(owner * half + s * n, n), n)

    def by_width(u, run):
        c = lax.rem(u, tiles)
        if last == wide:
            run(wide)
            return

        @pl.when(c != tiles - 1)
        def _():
            run(wide)

        @pl.when(c == tiles - 1)
        def _():
            run(last)

    def remote(src, dst, send, recv, to):
        return pltpu.make_async_remote_copy(
            src_ref=src, dst_ref=dst, send_sem=send, recv_sem=recv, device_id=to,
            device_id_type=pl.DeviceIdType.MESH)

    def x_local(s, part):
        return pltpu.make_async_copy(
            x.at[rows_of(s, part)], xg.at[s, pl.ds(part * n, n), pl.ds(0, depth)], x_own.at[s, part])

    def x_remote(s, part, k):
        return remote(
            x.at[rows_of(s, part)], xg.at[s, pl.ds(part * n, n), pl.ds((4 - k) * depth, depth)],
            x_send.at[s, part, k - 1], x_recv.at[s, part, 3 - k], {"b": peers[k]})

    def w_copies(u, width):
        slot = lax.rem(u, WEIGHTS)
        start = lax.rem(u, tiles) * wide
        columns = pl.ds(pl.multiple_of(start, LANES), width)
        copies = []
        for k in range(4):
            deep = pl.ds(pl.multiple_of(peers[k] * depth, depth), depth)
            for i, w in enumerate((wg, wu)):
                copies.append(pltpu.make_async_copy(
                    w.at[deep, columns],
                    wbuf.at[slot, pl.ds(k * depth, depth), pl.ds(i * width, width)], w_sem.at[slot, k, i]))
        return copies

    def d_copies(u, width):
        slot = lax.rem(u, WEIGHTS)
        start = lax.rem(u, tiles) * wide
        deep = pl.ds(pl.multiple_of(start, LANES), width)
        return [
            pltpu.make_async_copy(
                wd.at[deep, pl.ds(pl.multiple_of(peers[k] * cut, cut), cut)],
                dbuf.at[slot, k, pl.ds(0, width)], d_sem.at[slot, k])
            for k in range(4)]

    def start_all(copies):
        for copy in copies:
            copy.start()

    def wait_all(copies):
        for copy in copies:
            copy.wait()

    def p_copy(u, width):
        slot = lax.rem(u, RING)
        return remote(psend.at[slot, :, pl.ds(0, 2 * width)], precv.at[slot, :, pl.ds(0, 2 * width)],
                      p_send.at[slot], p_recv.at[slot], partner)

    def q_copy(u, width):
        slot = lax.rem(u, RING)
        return remote(hbuf.at[slot, pl.ds(0, n), pl.ds(0, width)], hbuf.at[slot, pl.ds(n, n), pl.ds(0, width)],
                      q_send.at[slot], q_recv.at[slot], partner)

    def y_copy(s, k):
        return remote(ysend.at[k - 1], yrecv.at[lax.rem(s, 2), 3 - k],
                      y_send.at[k - 1], y_recv.at[lax.rem(s, 2), 3 - k], {"b": peers[k]})

    def o_copy(s, part):
        return pltpu.make_async_copy(yout.at[pl.ds(part * n, n)], out.at[rows_of(s, part)], o_sem.at[part])

    def partial_sums(t):
        s, c = t // tiles, lax.rem(t, tiles)

        @pl.when(t + WEIGHTS - 1 < steps)
        def _():
            by_width(t + WEIGHTS - 1, lambda width: start_all(w_copies(t + WEIGHTS - 1, width)))

        @pl.when(c == 0)
        def _():
            for part in range(2):
                x_local(s, part).wait()
                for k in range(1, 4):
                    x_remote(s, part, k).wait_recv()

        @pl.when(t >= RING)
        def _():
            by_width(t - RING, lambda width: p_copy(t - RING, width).wait_send())

        def run(width):
            wait_all(w_copies(t, width))
            total = dot(xg[s], wbuf[lax.rem(t, WEIGHTS), :, : 2 * width])
            psend[lax.rem(t, RING), :, : 2 * width] = total[n:].astype(BF16)
            mine[lax.rem(t, KEPT), :, : 2 * width] = total[:n]
            p_copy(t, width).start()

        by_width(t, run)

    def hidden(u):
        @pl.when(u >= RING)
        def _():
            by_width(u - RING, lambda width: q_copy(u - RING, width).wait_send())

        def run(width):
            p_copy(u, width).wait_recv()
            slot, kept = lax.rem(u, RING), lax.rem(u, KEPT)
            gate = mine[kept, :, :width] + precv[slot, :, :width].astype(F32)
            up = mine[kept, :, width : 2 * width] + precv[slot, :, width : 2 * width].astype(F32)
            hbuf[slot, :n, :width] = (jax.nn.silu(gate) * up).astype(BF16)
            q_copy(u, width).start()

        by_width(u, run)

    def hand_out(s):
        @pl.when(s > 0)
        def _():
            for k in range(1, 4):
                y_copy(s - 1, k).wait_send()

        for k in range(1, 4):
            ysend[k - 1] = acc[k].astype(BF16)
            y_copy(s, k).start()
        yown[...] = acc[0]
        acc[...] = jnp.zeros_like(acc)

    def finish(s):
        for k in range(1, 4):
            y_copy(s, k).wait_recv()

        @pl.when(s > 0)
        def _():
            for part in range(2):
                o_copy(s - 1, part).wait()

        slot = lax.rem(s, 2)
        total = yown[...]
        for k in range(3):
            total = total + yrecv[slot, k].astype(F32)
        yout[...] = total.astype(BF16)
        for part in range(2):
            o_copy(s, part).start()

    def down(u):
        s, c = u // tiles, lax.rem(u, tiles)

        @pl.when(u + WEIGHTS - 1 < steps)
        def _():
            by_width(u + WEIGHTS - 1, lambda width: start_all(d_copies(u + WEIGHTS - 1, width)))

        def run(width):
            wait_all(d_copies(u, width))
            q_copy(u, width).wait_recv()
            h = hbuf[lax.rem(u, RING), :, :width]
            for k in range(4):
                acc[k] += dot(h, dbuf[lax.rem(u, WEIGHTS), k, :width])

        by_width(u, run)

        @pl.when(c == tiles - 1)
        def _():
            hand_out(s)

        @pl.when((c == tiles // 2) & (s > 0))
        def _():
            finish(s - 1)

    barrier = pltpu.get_barrier_semaphore()
    for to in [partner] + [{"b": peers[k]} for k in range(1, 4)]:
        pl.semaphore_signal(barrier, inc=1, device_id=to, device_id_type=pl.DeviceIdType.MESH)
    for u in range(WEIGHTS - 1):
        start_all(w_copies(u, wide))
        start_all(d_copies(u, wide))

    def own(s, _):
        for part in range(2):
            x_local(s, part).start()
        return 0

    lax.fori_loop(0, blocks, own, 0)
    acc[...] = jnp.zeros_like(acc)
    pl.semaphore_wait(barrier, 4)

    def others(s, _):
        for part in range(2):
            for k in range(1, 4):
                x_remote(s, part, k).start()
        return 0

    lax.fori_loop(0, blocks, others, 0)

    def step(t, _):
        @pl.when(t < steps)
        def _():
            partial_sums(t)

        @pl.when((t >= LAG_E) & (t < steps + LAG_E))
        def _():
            hidden(t - LAG_E)

        @pl.when(t >= LAG_D)
        def _():
            down(t - LAG_D)

        return 0

    lax.fori_loop(0, steps + LAG_D, step, 0)
    finish(blocks - 1)
    for part in range(2):
        o_copy(blocks - 1, part).wait()
    for k in range(1, 4):
        y_copy(blocks - 1, k).wait_send()
    for u in range(steps - RING, steps):
        width = last if u % tiles == tiles - 1 else wide
        p_copy(u, width).wait_send()
        q_copy(u, width).wait_send()

    def sent(s, _):
        for part in range(2):
            for k in range(1, 4):
                x_remote(s, part, k).wait_send()
        return 0

    lax.fori_loop(0, blocks, sent, 0)


def solution(mesh, n=BLOCK, wide=WIDE):
    def body(x, w_gate, w_up, w_down):
        rows, depth = x.shape
        blocks = rows // 2 // n
        dma = pltpu.SemaphoreType.DMA
        return pl.pallas_call(
            functools.partial(kernel, n, wide),
            out_shape=jax.ShapeDtypeStruct(x.shape, BF16),
            in_specs=[pl.BlockSpec(memory_space=pl.ANY)] * 4,
            out_specs=pl.BlockSpec(memory_space=pl.ANY),
            scratch_shapes=[
                pltpu.VMEM((blocks, 2 * n, 4 * depth), BF16),
                pltpu.VMEM((WEIGHTS, 4 * depth, 2 * wide), BF16),
                pltpu.VMEM((WEIGHTS, 4, wide, depth), BF16),
                pltpu.VMEM((4, 2 * n, depth), F32),
                pltpu.VMEM((KEPT, n, 2 * wide), F32),
                pltpu.VMEM((RING, n, 2 * wide), BF16),
                pltpu.VMEM((RING, n, 2 * wide), BF16),
                pltpu.VMEM((RING, 2 * n, wide), BF16),
                pltpu.VMEM((3, 2 * n, depth), BF16),
                pltpu.VMEM((2, 3, 2 * n, depth), BF16),
                pltpu.VMEM((2 * n, depth), F32),
                pltpu.VMEM((2 * n, depth), BF16),
                dma((blocks, 2)), dma((blocks, 2, 3)), dma((blocks, 2, 3)),
                dma((WEIGHTS, 4, 2)), dma((WEIGHTS, 4)),
                dma((RING,)), dma((RING,)), dma((RING,)), dma((RING,)),
                dma((3,)), dma((2, 3)), dma((2,)),
            ],
            compiler_params=pltpu.CompilerParams(
                collective_id=0, has_side_effects=True, vmem_limit_bytes=67_000_000),
        )(x, w_gate, w_up, w_down)

    return jax.shard_map(
        body,
        mesh=mesh,
        in_specs=(P("dp", ("a", "b")), P("a", "b"), P("a", "b"), P("b", "a")),
        out_specs=P("dp", ("a", "b")),
        check_vma=False,
    )
```

```python
import functools

import jax
import jax.numpy as jnp
from jax import lax
from jax.experimental import pallas as pl
from jax.experimental.pallas import tpu as pltpu
from jax.sharding import PartitionSpec as P

BLOCK = 128
WIDE = 256
LANES = 128
LAG_E, LAG_D = 3, 6
RING = 8
KEPT = LAG_E + 1
WEIGHTS = 3
F32, BF16 = jnp.float32, jnp.bfloat16


def dot(p, q):
    return jnp.dot(p, q, preferred_element_type=F32)


def kernel(n, wide, x, wg, wu, wd, out, xg, wbuf, dbuf, acc, mine, psend, precv, hbuf, ysend, yrecv, zsend, zrecv,
           yown, ykeep, yout, x_own, x_send, x_recv, w_sem, d_sem, p_send, p_recv, q_send, q_recv, y_send, y_recv,
           z_send, z_recv, o_sem):
    rows, depth = x.shape
    ff = wg.shape[1]
    half = rows // 2
    small = n // 2
    blocks = half // n + 1
    tiles = -(-ff // wide)
    last = ff - (tiles - 1) * wide
    steps = blocks * tiles
    cut = depth
    a, b = lax.axis_index("a"), lax.axis_index("b")
    chip, core = b // 2, lax.rem(b, 2)
    peers = [b, chip * 2 + 1 - core, (1 - chip) * 2 + core, (1 - chip) * 2 + 1 - core]
    partner, mate, across = {"a": 1 - a}, {"b": peers[1]}, {"b": peers[2]}

    def first_row(s):
        return s * n - small * ((s + blocks - 1) // blocks)

    def rows_of(s, part, size):
        owner = a if part == 0 else 1 - a
        return pl.ds(pl.multiple_of(owner * half + first_row(s), small), size)

    def held(s, start, size):
        return pl.ds(pl.multiple_of(2 * first_row(s) + start, small), size)

    def by_rows(s, run):
        if isinstance(s, int):
            return run(small if s in (0, blocks - 1) else n)
        ends = (s == 0) | (s == blocks - 1)

        @pl.when(ends)
        def _():
            run(small)

        @pl.when(jnp.logical_not(ends))
        def _():
            run(n)

    def by_width(u, run):
        if isinstance(u, int):
            return run(last if u % tiles == tiles - 1 else wide)
        c = lax.rem(u, tiles)
        if last == wide:
            return run(wide)

        @pl.when(c != tiles - 1)
        def _():
            run(wide)

        @pl.when(c == tiles - 1)
        def _():
            run(last)

    def by_shape(u, run):
        by_rows(u // tiles, lambda size: by_width(u, lambda width: run(size, width)))

    def remote(src, dst, send, recv, to):
        return pltpu.make_async_remote_copy(
            src_ref=src, dst_ref=dst, send_sem=send, recv_sem=recv, device_id=to,
            device_id_type=pl.DeviceIdType.MESH)

    def x_copy(s, part, k, size):
        to = held(s, part * size, size)
        if k == 0:
            return pltpu.make_async_copy(x.at[rows_of(s, part, size)], xg.at[to, pl.ds(0, depth)], x_own.at[s, part])
        src = xg.at[to, pl.ds(2 * depth, depth)] if k == 3 else x.at[rows_of(s, part, size)]
        return remote(src, xg.at[to, pl.ds(k * depth, depth)], x_send.at[s, part, k - 1], x_recv.at[s, part, k - 1],
                      across if k == 2 else mate)

    def x_start(s, k):
        by_rows(s, lambda size: [x_copy(s, part, k, size).start() for part in range(2)])

    def x_forward(s):
        def run(size):
            for part in range(2):
                x_copy(s, part, 2, size).wait_recv()
                x_copy(s, part, 3, size).start()

        by_rows(s, run)

    def w_copies(u, width):
        slot = lax.rem(u, WEIGHTS)
        start = lax.rem(u, tiles) * wide
        columns = pl.ds(pl.multiple_of(start, LANES), width)
        copies = []
        for k in range(4):
            deep = pl.ds(pl.multiple_of(peers[k] * depth, depth), depth)
            for i, w in enumerate((wg, wu)):
                copies.append(pltpu.make_async_copy(
                    w.at[deep, columns],
                    wbuf.at[slot, pl.ds(k * depth, depth), pl.ds(i * width, width)], w_sem.at[slot, k, i]))
        return copies

    def d_copies(u, width):
        slot = lax.rem(u, WEIGHTS)
        start = lax.rem(u, tiles) * wide
        deep = pl.ds(pl.multiple_of(start, LANES), width)
        return [
            pltpu.make_async_copy(
                wd.at[deep, pl.ds(pl.multiple_of(peers[k] * cut, cut), cut)],
                dbuf.at[slot, k, pl.ds(0, width)], d_sem.at[slot, k])
            for k in range(4)]

    def start_all(copies):
        for copy in copies:
            copy.start()

    def wait_all(copies):
        for copy in copies:
            copy.wait()

    def p_copy(u, size, width):
        slot = lax.rem(u, RING)
        part = (slot, pl.ds(0, size), pl.ds(0, 2 * width))
        return remote(psend.at[part], precv.at[part], p_send.at[slot], p_recv.at[slot], partner)

    def q_copy(u, size, width):
        slot = lax.rem(u, RING)
        return remote(hbuf.at[slot, pl.ds(0, size), pl.ds(0, width)], hbuf.at[slot, pl.ds(size, size), pl.ds(0, width)],
                      q_send.at[slot], q_recv.at[slot], partner)

    def y_copy(s, i, size):
        slot = lax.rem(s, 2)
        return remote(ysend.at[i, pl.ds(0, 2 * size)], yrecv.at[slot, i, pl.ds(0, 2 * size)],
                      y_send.at[i], y_recv.at[slot, i], mate)

    def z_copy(s, size):
        slot = lax.rem(s, 2)
        return remote(zsend.at[pl.ds(0, 2 * size)], zrecv.at[slot, pl.ds(0, 2 * size)], z_send, z_recv.at[slot], across)

    def o_copy(s, part, size):
        return pltpu.make_async_copy(yout.at[pl.ds(part * size, size)], out.at[rows_of(s, part, size)], o_sem.at[part])

    def partial_sums(t):
        s, c = t // tiles, lax.rem(t, tiles)

        @pl.when(t + WEIGHTS - 1 < steps)
        def _():
            by_width(t + WEIGHTS - 1, lambda width: start_all(w_copies(t + WEIGHTS - 1, width)))

        @pl.when((c == tiles // 2) & (s + 1 < blocks))
        def _():
            x_forward(s + 1)

        @pl.when(c == 0)
        def _():
            def run(size):
                for part in range(2):
                    x_copy(s, part, 0, size).wait()
                    x_copy(s, part, 1, size).wait_recv()
                    x_copy(s, part, 3, size).wait_recv()

            by_rows(s, run)

        @pl.when(t >= RING)
        def _():
            by_shape(t - RING, lambda size, width: p_copy(t - RING, size, width).wait_send())
            by_shape(t - RING, lambda size, width: q_copy(t - RING, size, width).wait_send())

        def run(size, width):
            wait_all(w_copies(t, width))
            total = dot(xg[held(s, 0, 2 * size)], wbuf[lax.rem(t, WEIGHTS), :, : 2 * width])
            psend[lax.rem(t, RING), :size, : 2 * width] = total[size:].astype(BF16)
            mine[lax.rem(t, KEPT), :size, : 2 * width] = total[:size]
            p_copy(t, size, width).start()

        by_shape(t, run)

    def hidden(u):
        def run(size, width):
            p_copy(u, size, width).wait_recv()
            slot, kept = lax.rem(u, RING), lax.rem(u, KEPT)
            gate = mine[kept, :size, :width] + precv[slot, :size, :width].astype(F32)
            up = mine[kept, :size, width : 2 * width] + precv[slot, :size, width : 2 * width].astype(F32)
            hbuf[slot, :size, :width] = (jax.nn.silu(gate) * up).astype(BF16)
            q_copy(u, size, width).start()

        by_shape(u, run)

    def hand_out(s):
        @pl.when(s > 0)
        def _():
            by_rows(s - 1, lambda size: [y_copy(s - 1, i, size).wait_send() for i in range(2)])

        def run(size):
            for i in (1, 0):
                ysend[i, : 2 * size] = acc[2 * i + 1, : 2 * size].astype(BF16)
                y_copy(s, i, size).start()
            yown[: 2 * size] = acc[0, : 2 * size]
            ykeep[: 2 * size] = acc[2, : 2 * size]

        by_rows(s, run)
        acc[...] = jnp.zeros_like(acc)

    def pass_on(s):
        def run(size):
            y_copy(s, 1, size).wait_recv()
            total = ykeep[: 2 * size] + yrecv[lax.rem(s, 2), 1, : 2 * size].astype(F32)
            zsend[: 2 * size] = total.astype(BF16)
            z_copy(s, size).start()

        by_rows(s, run)

    def finish(s):
        def written(size):
            for part in range(2):
                o_copy(s - 1, part, size).wait()

        if isinstance(s, int):
            by_rows(s - 1, written)
        else:
            pl.when(s > 0)(lambda: by_rows(s - 1, written))

        def run(size):
            slot = lax.rem(s, 2)
            y_copy(s, 0, size).wait_recv()
            total = yown[: 2 * size] + yrecv[slot, 0, : 2 * size].astype(F32)
            z_copy(s, size).wait_recv()
            yout[: 2 * size] = (total + zrecv[slot, : 2 * size].astype(F32)).astype(BF16)
            for part in range(2):
                o_copy(s, part, size).start()
            z_copy(s, size).wait_send()

        by_rows(s, run)

    def down(u):
        s, c = u // tiles, lax.rem(u, tiles)

        @pl.when(u + WEIGHTS - 1 < steps)
        def _():
            by_width(u + WEIGHTS - 1, lambda width: start_all(d_copies(u + WEIGHTS - 1, width)))

        def run(size, width):
            wait_all(d_copies(u, width))
            q_copy(u, size, width).wait_recv()
            h = hbuf[lax.rem(u, RING), : 2 * size, :width]
            for k in range(4):
                acc[k, : 2 * size] += dot(h, dbuf[lax.rem(u, WEIGHTS), k, :width])

        by_shape(u, run)

        @pl.when(c == tiles - 1)
        def _():
            hand_out(s)

        @pl.when((c == 1) & (s > 0))
        def _():
            pass_on(s - 1)

        @pl.when((c == tiles // 2) & (s > 0))
        def _():
            finish(s - 1)

    barrier = pltpu.get_barrier_semaphore()
    for to in (partner, mate, across):
        pl.semaphore_signal(barrier, inc=1, device_id=to, device_id_type=pl.DeviceIdType.MESH)

    def each(low, run):
        def one(s, _):
            run(s)
            return 0

        lax.fori_loop(low, blocks, one, 0)

    each(0, lambda s: x_start(s, 0))
    for u in range(WEIGHTS - 1):
        start_all(w_copies(u, wide))
    acc[...] = jnp.zeros_like(acc)
    pl.semaphore_wait(barrier, 3)
    x_start(0, 2)
    x_start(0, 1)
    each(1, lambda s: x_start(s, 2))
    for u in range(WEIGHTS - 1):
        start_all(d_copies(u, wide))
    x_forward(0)
    each(1, lambda s: x_start(s, 1))

    def step(t, _):
        @pl.when(t < steps)
        def _():
            partial_sums(t)

        @pl.when((t >= LAG_E) & (t < steps + LAG_E))
        def _():
            hidden(t - LAG_E)

        @pl.when(t >= LAG_D)
        def _():
            down(t - LAG_D)

        return 0

    lax.fori_loop(0, steps + LAG_D, step, 0)
    end = blocks - 1
    pass_on(end)
    finish(end)
    for part in range(2):
        o_copy(end, part, small).wait()
    for i in range(2):
        y_copy(end, i, small).wait_send()
    for u in range(steps - RING, steps):
        by_shape(u, lambda size, width: p_copy(u, size, width).wait_send())
        by_shape(u, lambda size, width: q_copy(u, size, width).wait_send())
    for k in range(1, 4):
        each(0, lambda s: by_rows(s, lambda size: [x_copy(s, part, k, size).wait_send() for part in range(2)]))


def solution(mesh, n=BLOCK, wide=WIDE):
    def body(x, w_gate, w_up, w_down):
        rows, depth = x.shape
        blocks = rows // 2 // n + 1
        dma = pltpu.SemaphoreType.DMA
        return pl.pallas_call(
            functools.partial(kernel, n, wide),
            out_shape=jax.ShapeDtypeStruct(x.shape, BF16),
            in_specs=[pl.BlockSpec(memory_space=pl.ANY)] * 4,
            out_specs=pl.BlockSpec(memory_space=pl.ANY),
            scratch_shapes=[
                pltpu.VMEM((rows, 4 * depth), BF16),
                pltpu.VMEM((WEIGHTS, 4 * depth, 2 * wide), BF16),
                pltpu.VMEM((WEIGHTS, 4, wide, depth), BF16),
                pltpu.VMEM((4, 2 * n, depth), F32),
                pltpu.VMEM((KEPT, n, 2 * wide), F32),
                pltpu.VMEM((RING, n, 2 * wide), BF16),
                pltpu.VMEM((RING, n, 2 * wide), BF16),
                pltpu.VMEM((RING, 2 * n, wide), BF16),
                pltpu.VMEM((2, 2 * n, depth), BF16),
                pltpu.VMEM((2, 2, 2 * n, depth), BF16),
                pltpu.VMEM((2 * n, depth), BF16),
                pltpu.VMEM((2, 2 * n, depth), BF16),
                pltpu.VMEM((2 * n, depth), F32),
                pltpu.VMEM((2 * n, depth), F32),
                pltpu.VMEM((2 * n, depth), BF16),
                dma((blocks, 2)), dma((blocks, 2, 3)), dma((blocks, 2, 3)),
                dma((WEIGHTS, 4, 2)), dma((WEIGHTS, 4)),
                dma((RING,)), dma((RING,)), dma((RING,)), dma((RING,)),
                dma((2,)), dma((2, 2)), dma, dma((2,)), dma((2,)),
            ],
            compiler_params=pltpu.CompilerParams(
                collective_id=0, has_side_effects=True, vmem_limit_bytes=67_000_000),
        )(x, w_gate, w_up, w_down)

    return jax.shard_map(
        body,
        mesh=mesh,
        in_specs=(P("dp", ("a", "b")), P("a", "b"), P("a", "b"), P("b", "a")),
        out_specs=P("dp", ("a", "b")),
        check_vma=False,
    )
```

```python
import functools

import jax
import jax.numpy as jnp
from jax import lax
from jax.experimental import pallas as pl
from jax.experimental.pallas import tpu as pltpu
from jax.sharding import PartitionSpec as P

BLOCK = 128
WIDE = 256
LANES = 128
LAG_E, LAG_D = 3, 6
RING = 8
KEPT = LAG_E + 1
EARLY = 2
WEIGHTS = 3
F32, BF16 = jnp.float32, jnp.bfloat16


def dot(p, q):
    return jnp.dot(p, q, preferred_element_type=F32)


def kernel(n, wide, x, wg, wu, wd, out, xg, wbuf, dbuf, acc, mine, psend, precv, hbuf, ysend, yrecv, zsend, zrecv,
           yown, ykeep, x_own, x_send, x_recv, w_sem, d_sem, p_send, p_recv, q_send, q_recv, y_send, y_recv,
           z_send, z_recv):
    rows, depth = x.shape
    ff = wg.shape[1]
    half = rows // 2
    small = n // 2
    blocks = half // n + 1
    tiles = -(-ff // wide)
    last = ff - (tiles - 1) * wide
    steps = blocks * tiles
    cut = depth
    a, b = lax.axis_index("a"), lax.axis_index("b")
    chip, core = b // 2, lax.rem(b, 2)
    peers = [b, chip * 2 + 1 - core, (1 - chip) * 2 + core, (1 - chip) * 2 + 1 - core]
    partner, mate, across = {"a": 1 - a}, {"b": peers[1]}, {"b": peers[2]}

    def first_row(s):
        return s * n - small * ((s + blocks - 1) // blocks)

    def rows_of(s, part, size):
        owner = a if part == 0 else 1 - a
        return pl.ds(pl.multiple_of(owner * half + first_row(s), small), size)

    def held(s, start, size):
        return pl.ds(pl.multiple_of(2 * first_row(s) + start, small), size)

    def by_rows(s, run):
        if isinstance(s, int):
            return run(small if s in (0, blocks - 1) else n)
        ends = (s == 0) | (s == blocks - 1)

        @pl.when(ends)
        def _():
            run(small)

        @pl.when(jnp.logical_not(ends))
        def _():
            run(n)

    def by_width(u, run):
        if isinstance(u, int):
            return run(last if u % tiles == tiles - 1 else wide)
        c = lax.rem(u, tiles)
        if last == wide:
            return run(wide)

        @pl.when(c != tiles - 1)
        def _():
            run(wide)

        @pl.when(c == tiles - 1)
        def _():
            run(last)

    def by_shape(u, run):
        by_rows(u // tiles, lambda size: by_width(u, lambda width: run(size, width)))

    def remote(src, dst, send, recv, to):
        return pltpu.make_async_remote_copy(
            src_ref=src, dst_ref=dst, send_sem=send, recv_sem=recv, device_id=to,
            device_id_type=pl.DeviceIdType.MESH)

    def x_copy(s, part, k, size):
        to = held(s, part * size, size)
        if k == 0:
            return pltpu.make_async_copy(x.at[rows_of(s, part, size)], xg.at[to, pl.ds(0, depth)], x_own.at[s, part])
        src = xg.at[to, pl.ds(2 * depth, depth)] if k == 3 else x.at[rows_of(s, part, size)]
        return remote(src, xg.at[to, pl.ds(k * depth, depth)], x_send.at[s, part, k - 1], x_recv.at[s, part, k - 1],
                      across if k == 2 else mate)

    def x_start(s, k, parts=(0, 1)):
        by_rows(s, lambda size: [x_copy(s, part, k, size).start() for part in parts])

    def x_forward(s, parts=(0, 1)):
        def run(size):
            for part in parts:
                x_copy(s, part, 2, size).wait_recv()
                x_copy(s, part, 3, size).start()

        by_rows(s, run)

    def x_ready(s, parts=(0, 1)):
        def run(size):
            for part in parts:
                x_copy(s, part, 0, size).wait()
                x_copy(s, part, 1, size).wait_recv()
                x_copy(s, part, 3, size).wait_recv()

        by_rows(s, run)

    def w_copies(u, width):
        slot = lax.rem(u, WEIGHTS)
        start = lax.rem(u, tiles) * wide
        columns = pl.ds(pl.multiple_of(start, LANES), width)
        copies = []
        for k in range(4):
            deep = pl.ds(pl.multiple_of(peers[k] * depth, depth), depth)
            for i, w in enumerate((wg, wu)):
                copies.append(pltpu.make_async_copy(
                    w.at[deep, columns],
                    wbuf.at[slot, pl.ds(k * depth, depth), pl.ds(i * width, width)], w_sem.at[slot, k, i]))
        return copies

    def d_copies(u, width):
        slot = lax.rem(u, WEIGHTS)
        start = lax.rem(u, tiles) * wide
        deep = pl.ds(pl.multiple_of(start, LANES), width)
        return [
            pltpu.make_async_copy(
                wd.at[deep, pl.ds(pl.multiple_of(peers[k] * cut, cut), cut)],
                dbuf.at[slot, k, pl.ds(0, width)], d_sem.at[slot, k])
            for k in range(4)]

    def start_all(copies):
        for copy in copies:
            copy.start()

    def wait_all(copies):
        for copy in copies:
            copy.wait()

    def p_copy(u, size, width):
        slot = lax.rem(u, RING)
        part = (slot, pl.ds(0, size), pl.ds(0, 2 * width))
        return remote(psend.at[part], precv.at[part], p_send.at[slot], p_recv.at[slot], partner)

    def q_copy(u, size, width):
        slot = lax.rem(u, RING)
        return remote(hbuf.at[slot, pl.ds(0, size), pl.ds(0, width)], hbuf.at[slot, pl.ds(size, size), pl.ds(0, width)],
                      q_send.at[slot], q_recv.at[slot], partner)

    def y_copy(s, i, size):
        slot = lax.rem(s, 2)
        to = pl.ds(0, 2 * size) if i == 0 else pl.ds((i - 1) * size, size)
        return remote(ysend.at[min(i, 1), to], yrecv.at[slot, min(i, 1), to], y_send.at[i], y_recv.at[slot, i], mate)

    def z_copy(s, part, size):
        slot = lax.rem(s, 2)
        to = pl.ds(part * size, size)
        return remote(zsend.at[to], zrecv.at[slot, to], z_send.at[part], z_recv.at[slot, part], across)

    def partial_sums(t):
        s, c = t // tiles, lax.rem(t, tiles)

        @pl.when((t > EARLY) & (t + WEIGHTS - 1 < steps))
        def _():
            by_width(t + WEIGHTS - 1, lambda width: start_all(w_copies(t + WEIGHTS - 1, width)))

        @pl.when((c == tiles // 2) & (s + 1 < blocks))
        def _():
            x_forward(s + 1)

        @pl.when(c == 0)
        def _():
            x_ready(s)

        @pl.when(t >= RING)
        def _():
            by_shape(t - RING, lambda size, width: p_copy(t - RING, size, width).wait_send())
            by_shape(t - RING, lambda size, width: q_copy(t - RING, size, width).wait_send())

        def run(size, width):
            wait_all(w_copies(t, width))
            total = dot(xg[held(s, 0, 2 * size)], wbuf[lax.rem(t, WEIGHTS), :, : 2 * width])
            psend[lax.rem(t, RING), :size, : 2 * width] = total[size:].astype(BF16)
            mine[lax.rem(t, KEPT), :size, : 2 * width] = total[:size]
            p_copy(t, size, width).start()

        by_shape(t, run)

    def early_sums(t, part):
        def run(size, width):
            if part:
                wait_all(w_copies(t, width))
            total = dot(xg[held(0, part * size, size)], wbuf[t, :, : 2 * width])
            if part:
                psend[t, :size, : 2 * width] = total.astype(BF16)
                p_copy(t, size, width).start()
            else:
                mine[t, :size, : 2 * width] = total

        by_shape(t, run)

    def hidden(u):
        def run(size, width):
            p_copy(u, size, width).wait_recv()
            slot, kept = lax.rem(u, RING), lax.rem(u, KEPT)
            gate = mine[kept, :size, :width] + precv[slot, :size, :width].astype(F32)
            up = mine[kept, :size, width : 2 * width] + precv[slot, :size, width : 2 * width].astype(F32)
            hbuf[slot, :size, :width] = (jax.nn.silu(gate) * up).astype(BF16)
            q_copy(u, size, width).start()

        by_shape(u, run)

    def hand_out(s):
        @pl.when(s > 0)
        def _():
            by_rows(s - 1, lambda size: [y_copy(s - 1, i, size).wait_send() for i in range(3)])

        def run(size):
            for part in range(2):
                to = pl.ds(part * size, size)
                ysend[1, to] = acc[3, to].astype(BF16)
                y_copy(s, part + 1, size).start()
            ysend[0, : 2 * size] = acc[1, : 2 * size].astype(BF16)
            y_copy(s, 0, size).start()
            yown[: 2 * size] = acc[0, : 2 * size]
            ykeep[: 2 * size] = acc[2, : 2 * size]

        by_rows(s, run)
        acc[...] = jnp.zeros_like(acc)

    def pass_on(s):
        def run(size):
            for part in range(2):
                to = pl.ds(part * size, size)
                y_copy(s, part + 1, size).wait_recv()
                zsend[to] = (ykeep[to] + yrecv[lax.rem(s, 2), 1, to].astype(F32)).astype(BF16)
                z_copy(s, part, size).start()

        by_rows(s, run)

    def finish(s):
        def run(size):
            slot = lax.rem(s, 2)
            y_copy(s, 0, size).wait_recv()
            for part in range(2):
                to = pl.ds(part * size, size)
                z_copy(s, part, size).wait_recv()
                total = yown[to] + yrecv[slot, 0, to].astype(F32) + zrecv[slot, to].astype(F32)
                out[rows_of(s, part, size)] = total.astype(BF16)
            for part in range(2):
                z_copy(s, part, size).wait_send()

        by_rows(s, run)

    def down(u):
        s, c = u // tiles, lax.rem(u, tiles)

        @pl.when(u + WEIGHTS - 1 < steps)
        def _():
            by_width(u + WEIGHTS - 1, lambda width: start_all(d_copies(u + WEIGHTS - 1, width)))

        def run(size, width):
            wait_all(d_copies(u, width))
            q_copy(u, size, width).wait_recv()
            h = hbuf[lax.rem(u, RING), : 2 * size, :width]
            for k in range(4):
                acc[k, : 2 * size] += dot(h, dbuf[lax.rem(u, WEIGHTS), k, :width])

        by_shape(u, run)

        @pl.when(c == tiles - 1)
        def _():
            hand_out(s)

        @pl.when((c == 1) & (s > 0))
        def _():
            pass_on(s - 1)

        @pl.when((c == tiles // 2) & (s > 0))
        def _():
            finish(s - 1)

    barrier = pltpu.get_barrier_semaphore()
    for to in (partner, mate, across):
        pl.semaphore_signal(barrier, inc=1, device_id=to, device_id_type=pl.DeviceIdType.MESH)

    def each(low, run):
        def one(s, _):
            run(s)
            return 0

        lax.fori_loop(low, blocks, one, 0)

    each(0, lambda s: x_start(s, 0))
    for u in range(WEIGHTS):
        start_all(w_copies(u, wide))
    acc[...] = jnp.zeros_like(acc)
    pl.semaphore_wait(barrier, 3)
    for k in (2, 1):
        x_start(0, k, (1,))
    for k in (2, 1):
        x_start(0, k, (0,))
    x_forward(0, (1,))
    x_ready(0, (1,))
    early_sums(0, 1)
    x_forward(0, (0,))
    for u in range(1, EARLY):
        early_sums(u, 1)
    x_ready(0, (0,))
    for u in range(EARLY):
        early_sums(u, 0)
        start_all(w_copies(u + WEIGHTS, wide))
    for u in range(WEIGHTS - 1):
        start_all(d_copies(u, wide))
    each(1, lambda s: x_start(s, 2))
    each(1, lambda s: x_start(s, 1))

    def step(t, _):
        @pl.when(t < steps)
        def _():
            partial_sums(t)

        @pl.when((t >= LAG_E) & (t < steps + LAG_E))
        def _():
            hidden(t - LAG_E)

        @pl.when(t >= LAG_D)
        def _():
            down(t - LAG_D)

        return 0

    lax.fori_loop(EARLY, steps + LAG_D, step, 0)
    end = blocks - 1
    pass_on(end)
    finish(end)
    for i in range(3):
        y_copy(end, i, small).wait_send()
    for u in range(steps - RING, steps):
        by_shape(u, lambda size, width: p_copy(u, size, width).wait_send())
        by_shape(u, lambda size, width: q_copy(u, size, width).wait_send())
    for k in range(1, 4):
        each(0, lambda s: by_rows(s, lambda size: [x_copy(s, part, k, size).wait_send() for part in range(2)]))


def solution(mesh, n=BLOCK, wide=WIDE):
    def body(x, w_gate, w_up, w_down):
        rows, depth = x.shape
        blocks = rows // 2 // n + 1
        dma = pltpu.SemaphoreType.DMA
        return pl.pallas_call(
            functools.partial(kernel, n, wide),
            out_shape=pltpu.VMEM(x.shape, BF16),
            in_specs=[pl.BlockSpec(memory_space=pl.ANY)] * 4,
            out_specs=pl.BlockSpec(memory_space=pltpu.VMEM),
            scratch_shapes=[
                pltpu.VMEM((rows, 4 * depth), BF16),
                pltpu.VMEM((WEIGHTS, 4 * depth, 2 * wide), BF16),
                pltpu.VMEM((WEIGHTS, 4, wide, depth), BF16),
                pltpu.VMEM((4, 2 * n, depth), F32),
                pltpu.VMEM((KEPT, n, 2 * wide), F32),
                pltpu.VMEM((RING, n, 2 * wide), BF16),
                pltpu.VMEM((RING, n, 2 * wide), BF16),
                pltpu.VMEM((RING, 2 * n, wide), BF16),
                pltpu.VMEM((2, 2 * n, depth), BF16),
                pltpu.VMEM((2, 2, 2 * n, depth), BF16),
                pltpu.VMEM((2 * n, depth), BF16),
                pltpu.VMEM((2, 2 * n, depth), BF16),
                pltpu.VMEM((2 * n, depth), F32),
                pltpu.VMEM((2 * n, depth), F32),
                dma((blocks, 2)), dma((blocks, 2, 3)), dma((blocks, 2, 3)),
                dma((WEIGHTS, 4, 2)), dma((WEIGHTS, 4)),
                dma((RING,)), dma((RING,)), dma((RING,)), dma((RING,)),
                dma((3,)), dma((2, 3)), dma((2,)), dma((2, 2)),
            ],
            compiler_params=pltpu.CompilerParams(
                collective_id=0, has_side_effects=True, vmem_limit_bytes=58_000_000),
        )(x, w_gate, w_up, w_down)

    return jax.shard_map(
        body,
        mesh=mesh,
        in_specs=(P("dp", ("a", "b")), P("a", "b"), P("a", "b"), P("b", "a")),
        out_specs=P("dp", ("a", "b")),
        check_vma=False,
    )
```

```python
import functools

import jax
import jax.numpy as jnp
from jax import lax
from jax.experimental import pallas as pl
from jax.experimental.pallas import tpu as pltpu
from jax.sharding import PartitionSpec as P

BLOCK = 128
WIDE = 256
LANES = 128
LAG_E, LAG_D = 3, 6
RING = 8
KEPT = LAG_E + 1
EARLY = 2
WEIGHTS = 3
F32, BF16 = jnp.float32, jnp.bfloat16


def dot(p, q):
    return jnp.dot(p, q, preferred_element_type=F32)


def kernel(n, wide, x, wg, wu, wd, out, xg, wbuf, dbuf, acc, mine, psend, precv, hbuf, ysend, yrecv, zsend, zrecv,
           yown, ykeep, x_own, x_send, x_recv, w_sem, d_sem, p_send, p_recv, q_send, q_recv, y_send, y_recv,
           z_send, z_recv):
    rows, depth = x.shape
    ff = wg.shape[1]
    half = rows // 2
    small = n // 2
    blocks = half // n + 1
    tiles = -(-ff // wide)
    last = ff - (tiles - 1) * wide
    steps = blocks * tiles
    cut = depth
    a, b = lax.axis_index("a"), lax.axis_index("b")
    chip, core = b // 2, lax.rem(b, 2)
    peers = [b, chip * 2 + 1 - core, (1 - chip) * 2 + core, (1 - chip) * 2 + 1 - core]
    partner, mate, across = {"a": 1 - a}, {"b": peers[1]}, {"b": peers[2]}

    def first_row(s):
        return s * n - small * ((s + blocks - 1) // blocks)

    def rows_of(s, part, size):
        owner = a if part == 0 else 1 - a
        return pl.ds(pl.multiple_of(owner * half + first_row(s), small), size)

    def held(s, start, size):
        return pl.ds(pl.multiple_of(2 * first_row(s) + start, small), size)

    def by_rows(s, run):
        if isinstance(s, int):
            return run(small if s in (0, blocks - 1) else n)
        ends = (s == 0) | (s == blocks - 1)

        @pl.when(ends)
        def _():
            run(small)

        @pl.when(jnp.logical_not(ends))
        def _():
            run(n)

    def by_width(u, run):
        if isinstance(u, int):
            return run(last if u % tiles == tiles - 1 else wide)
        c = lax.rem(u, tiles)
        if last == wide:
            return run(wide)

        @pl.when(c != tiles - 1)
        def _():
            run(wide)

        @pl.when(c == tiles - 1)
        def _():
            run(last)

    def by_shape(u, run):
        by_rows(u // tiles, lambda size: by_width(u, lambda width: run(size, width)))

    def remote(src, dst, send, recv, to):
        return pltpu.make_async_remote_copy(
            src_ref=src, dst_ref=dst, send_sem=send, recv_sem=recv, device_id=to,
            device_id_type=pl.DeviceIdType.MESH)

    def x_copy(s, part, k, size):
        to = held(s, part * size, size)
        if k == 0:
            return pltpu.make_async_copy(x.at[rows_of(s, part, size)], xg.at[to, pl.ds(0, depth)], x_own.at[s, part])
        src = xg.at[to, pl.ds(2 * depth, depth)] if k == 3 else x.at[rows_of(s, part, size)]
        return remote(src, xg.at[to, pl.ds(k * depth, depth)], x_send.at[s, part, k - 1], x_recv.at[s, part, k - 1],
                      across if k == 2 else mate)

    def x_start(s, k, parts=(0, 1)):
        by_rows(s, lambda size: [x_copy(s, part, k, size).start() for part in parts])

    def x_forward(s, parts=(0, 1)):
        def run(size):
            for part in parts:
                x_copy(s, part, 2, size).wait_recv()
                x_copy(s, part, 3, size).start()

        by_rows(s, run)

    def x_ready(s, parts=(0, 1)):
        def run(size):
            for part in parts:
                x_copy(s, part, 0, size).wait()
                x_copy(s, part, 1, size).wait_recv()
                x_copy(s, part, 3, size).wait_recv()

        by_rows(s, run)

    def w_copies(u, width):
        slot = lax.rem(u, WEIGHTS)
        start = lax.rem(u, tiles) * wide
        columns = pl.ds(pl.multiple_of(start, LANES), width)
        copies = []
        for k in range(4):
            deep = pl.ds(pl.multiple_of(peers[k] * depth, depth), depth)
            for i, w in enumerate((wg, wu)):
                copies.append(pltpu.make_async_copy(
                    w.at[deep, columns],
                    wbuf.at[slot, pl.ds(k * depth, depth), pl.ds(i * width, width)], w_sem.at[slot, k, i]))
        return copies

    def d_copies(u, width):
        slot = lax.rem(u, WEIGHTS)
        start = lax.rem(u, tiles) * wide
        deep = pl.ds(pl.multiple_of(start, LANES), width)
        return [
            pltpu.make_async_copy(
                wd.at[deep, pl.ds(pl.multiple_of(peers[k] * cut, cut), cut)],
                dbuf.at[slot, k, pl.ds(0, width)], d_sem.at[slot, k])
            for k in range(4)]

    def start_all(copies):
        for copy in copies:
            copy.start()

    def wait_all(copies):
        for copy in copies:
            copy.wait()

    def p_copy(u, size, width):
        slot = lax.rem(u, RING)
        part = (slot, pl.ds(0, size), pl.ds(0, 2 * width))
        return remote(psend.at[part], precv.at[part], p_send.at[slot], p_recv.at[slot], partner)

    def q_copy(u, size, width):
        slot = lax.rem(u, RING)
        return remote(hbuf.at[slot, pl.ds(0, size), pl.ds(0, width)], hbuf.at[slot, pl.ds(size, size), pl.ds(0, width)],
                      q_send.at[slot], q_recv.at[slot], partner)

    def y_copy(s, i, size):
        slot = lax.rem(s, 2)
        to = pl.ds(0, 2 * size) if i == 0 else pl.ds((i - 1) * size, size)
        return remote(ysend.at[min(i, 1), to], yrecv.at[slot, min(i, 1), to], y_send.at[i], y_recv.at[slot, i], mate)

    def z_copy(s, part, size):
        slot = lax.rem(s, 2)
        to = pl.ds(part * size, size)
        return remote(zsend.at[to], zrecv.at[slot, to], z_send.at[part], z_recv.at[slot, part], across)

    def partial_sums(t):
        s, c = t // tiles, lax.rem(t, tiles)

        @pl.when((t > EARLY) & (t + WEIGHTS - 1 < steps))
        def _():
            by_width(t + WEIGHTS - 1, lambda width: start_all(w_copies(t + WEIGHTS - 1, width)))

        @pl.when((c == tiles // 2) & (s + 1 < blocks))
        def _():
            x_forward(s + 1)

        @pl.when(c == 0)
        def _():
            x_ready(s)

        @pl.when(t >= RING)
        def _():
            by_shape(t - RING, lambda size, width: p_copy(t - RING, size, width).wait_send())
            by_shape(t - RING, lambda size, width: q_copy(t - RING, size, width).wait_send())

        def run(size, width):
            wait_all(w_copies(t, width))
            total = dot(xg[held(s, 0, 2 * size)], wbuf[lax.rem(t, WEIGHTS), :, : 2 * width])
            psend[lax.rem(t, RING), :size, : 2 * width] = total[size:].astype(BF16)
            mine[lax.rem(t, KEPT), :size, : 2 * width] = total[:size]
            p_copy(t, size, width).start()

        by_shape(t, run)

    def early_sums(t, part):
        def run(size, width):
            if part:
                wait_all(w_copies(t, width))
            total = dot(xg[held(0, part * size, size)], wbuf[t, :, : 2 * width])
            if part:
                psend[t, :size, : 2 * width] = total.astype(BF16)
                p_copy(t, size, width).start()
            else:
                mine[t, :size, : 2 * width] = total

        by_shape(t, run)

    def hidden(u):
        def run(size, width):
            p_copy(u, size, width).wait_recv()
            slot, kept = lax.rem(u, RING), lax.rem(u, KEPT)
            gate = mine[kept, :size, :width] + precv[slot, :size, :width].astype(F32)
            up = mine[kept, :size, width : 2 * width] + precv[slot, :size, width : 2 * width].astype(F32)
            hbuf[slot, :size, :width] = (jax.nn.silu(gate) * up).astype(BF16)
            q_copy(u, size, width).start()

        by_shape(u, run)

    def pass_on(s):
        def run(size):
            for part in range(2):
                to = pl.ds(part * size, size)
                y_copy(s, part + 1, size).wait_recv()
                zsend[to] = (ykeep[to] + yrecv[lax.rem(s, 2), 1, to].astype(F32)).astype(BF16)
                z_copy(s, part, size).start()

        by_rows(s, run)

    def finish(s):
        def run(size):
            slot = lax.rem(s, 2)
            y_copy(s, 0, size).wait_recv()
            for part in range(2):
                to = pl.ds(part * size, size)
                z_copy(s, part, size).wait_recv()
                total = yown[to] + yrecv[slot, 0, to].astype(F32) + zrecv[slot, to].astype(F32)
                out[rows_of(s, part, size)] = total.astype(BF16)
            for part in range(2):
                z_copy(s, part, size).wait_send()

        by_rows(s, run)

    def down(u):
        s, c = u // tiles, lax.rem(u, tiles)

        @pl.when(u + WEIGHTS - 1 < steps)
        def _():
            by_width(u + WEIGHTS - 1, lambda width: start_all(d_copies(u + WEIGHTS - 1, width)))

        def run(size, width):
            wait_all(d_copies(u, width))
            q_copy(u, size, width).wait_recv()
            h = hbuf[lax.rem(u, RING), : 2 * size, :width]

            def total(k):
                return acc[k, : 2 * size] + dot(h, dbuf[lax.rem(u, WEIGHTS), k, :width])

            if width == wide:
                for k in range(4):
                    acc[k, : 2 * size] = total(k)
                return
            across_sum = total(3).astype(BF16)
            for part in range(2):
                ysend[1, pl.ds(part * size, size)] = across_sum[part * size : (part + 1) * size]
                y_copy(s, part + 1, size).start()
            ysend[0, : 2 * size] = total(1).astype(BF16)
            y_copy(s, 0, size).start()
            ykeep[: 2 * size] = total(2)
            yown[: 2 * size] = total(0)
            acc[...] = jnp.zeros_like(acc)

        @pl.when((c == tiles - 1) & (s > 0))
        def _():
            by_rows(s - 1, lambda size: [y_copy(s - 1, i, size).wait_send() for i in range(3)])

        by_shape(u, run)

        @pl.when((c == 1) & (s > 0))
        def _():
            pass_on(s - 1)

        @pl.when((c == tiles // 2) & (s > 0))
        def _():
            finish(s - 1)

    barrier = pltpu.get_barrier_semaphore()
    for to in (partner, mate, across):
        pl.semaphore_signal(barrier, inc=1, device_id=to, device_id_type=pl.DeviceIdType.MESH)

    def each(low, run):
        def one(s, _):
            run(s)
            return 0

        lax.fori_loop(low, blocks, one, 0)

    each(0, lambda s: x_start(s, 0))
    for u in range(WEIGHTS):
        start_all(w_copies(u, wide))
    acc[...] = jnp.zeros_like(acc)
    pl.semaphore_wait(barrier, 3)
    for k in (2, 1):
        x_start(0, k, (1,))
    for k in (2, 1):
        x_start(0, k, (0,))
    x_forward(0, (1,))
    x_ready(0, (1,))
    early_sums(0, 1)
    x_forward(0, (0,))
    for u in range(1, EARLY):
        early_sums(u, 1)
    x_ready(0, (0,))
    for u in range(EARLY):
        early_sums(u, 0)
        start_all(w_copies(u + WEIGHTS, wide))
    for u in range(WEIGHTS - 1):
        start_all(d_copies(u, wide))
    each(1, lambda s: x_start(s, 2))
    each(1, lambda s: x_start(s, 1))

    def step(t, _):
        @pl.when(t < steps)
        def _():
            partial_sums(t)

        @pl.when((t >= LAG_E) & (t < steps + LAG_E))
        def _():
            hidden(t - LAG_E)

        @pl.when(t >= LAG_D)
        def _():
            down(t - LAG_D)

        return 0

    lax.fori_loop(EARLY, steps + LAG_D, step, 0)
    end = blocks - 1
    pass_on(end)
    for i in range(3):
        y_copy(end, i, small).wait_send()
    for u in range(steps - RING, steps):
        by_shape(u, lambda size, width: p_copy(u, size, width).wait_send())
        by_shape(u, lambda size, width: q_copy(u, size, width).wait_send())
    for k in range(1, 4):
        each(0, lambda s: by_rows(s, lambda size: [x_copy(s, part, k, size).wait_send() for part in range(2)]))
    finish(end)


def solution(mesh, n=BLOCK, wide=WIDE):
    def body(x, w_gate, w_up, w_down):
        rows, depth = x.shape
        blocks = rows // 2 // n + 1
        dma = pltpu.SemaphoreType.DMA
        return pl.pallas_call(
            functools.partial(kernel, n, wide),
            out_shape=pltpu.VMEM(x.shape, BF16),
            in_specs=[pl.BlockSpec(memory_space=pl.ANY)] * 4,
            out_specs=pl.BlockSpec(memory_space=pltpu.VMEM),
            scratch_shapes=[
                pltpu.VMEM((rows, 4 * depth), BF16),
                pltpu.VMEM((WEIGHTS, 4 * depth, 2 * wide), BF16),
                pltpu.VMEM((WEIGHTS, 4, wide, depth), BF16),
                pltpu.VMEM((4, 2 * n, depth), F32),
                pltpu.VMEM((KEPT, n, 2 * wide), F32),
                pltpu.VMEM((RING, n, 2 * wide), BF16),
                pltpu.VMEM((RING, n, 2 * wide), BF16),
                pltpu.VMEM((RING, 2 * n, wide), BF16),
                pltpu.VMEM((2, 2 * n, depth), BF16),
                pltpu.VMEM((2, 2, 2 * n, depth), BF16),
                pltpu.VMEM((2 * n, depth), BF16),
                pltpu.VMEM((2, 2 * n, depth), BF16),
                pltpu.VMEM((2 * n, depth), F32),
                pltpu.VMEM((2 * n, depth), F32),
                dma((blocks, 2)), dma((blocks, 2, 3)), dma((blocks, 2, 3)),
                dma((WEIGHTS, 4, 2)), dma((WEIGHTS, 4)),
                dma((RING,)), dma((RING,)), dma((RING,)), dma((RING,)),
                dma((3,)), dma((2, 3)), dma((2,)), dma((2, 2)),
            ],
            compiler_params=pltpu.CompilerParams(
                collective_id=0, has_side_effects=True, vmem_limit_bytes=58_000_000),
        )(x, w_gate, w_up, w_down)

    return jax.shard_map(
        body,
        mesh=mesh,
        in_specs=(P("dp", ("a", "b")), P("a", "b"), P("a", "b"), P("b", "a")),
        out_specs=P("dp", ("a", "b")),
        check_vma=False,
    )
```
